8 devices in a mesh: stage: 1 (over z), fsdp: 2 (over y), tp: 4 (over x, core).
Axes of the slice: x: 2, y: 2, z: 1, core: 2. Of those that a mesh axis runs over, the one named last changes fastest.
Arguments:
- weight: float32 [2, 8192, 3072], P('stage', 'fsdp', 'tp')
- momentum: float32 [2, 8192, 3072], P('stage', 'fsdp', 'tp')
- gradient: bfloat16 [2, 8192, 3072], P('stage', 'fsdp', 'tp')
- learn_rate: float32 [], replicated
- mom_coef: float32 [], replicated
- weight_decay: float32 [], replicated
Outputs:
- output 1: float32 [2, 8192, 3072], P('stage', 'fsdp', 'tp')
- output 2: float32 [2, 8192, 3072], P('stage', 'fsdp', 'tp')
All inputs are finite; a program needn't handle non-finite values.
Results may differ from the reference program's by a relative error of at most 0.0108.
Values are sent between devices in bfloat16 or wider.
A program may use at most 1 GiB of HBM per device.

```python
import jax
import jax.numpy as jnp
from jax import lax
import math

MATRICES = 2
ROW_DIM = 8192
COL_DIM = 3072
NS_STEPS = 5

COEF_A = 3.4445
COEF_B = -4.7750
COEF_C = 2.0315
NORM_EPS = 1e-7


def low_rank_draw(key, rank_dim):
    key_u, key_v, key_n = jax.random.split(key, 3)
    decay = jnp.exp(-0.35 * jnp.arange(rank_dim, dtype=jnp.float32))
    decay = decay / jnp.sqrt(jnp.mean(decay * decay))
    left = jax.random.normal(key_u, (MATRICES, ROW_DIM, rank_dim), jnp.float32) * decay
    right = jax.random.normal(key_v, (MATRICES, rank_dim, COL_DIM), jnp.float32)
    noise = jax.random.normal(key_n, (MATRICES, ROW_DIM, COL_DIM), jnp.float32)
    low_part = jnp.einsum('erk,ekc->erc', left, right) / math.sqrt(rank_dim)
    return low_part + 0.5 * noise


def setup_inputs(seed: int = 0, part: int = 0) -> dict:
    base_key = jax.random.key(seed)
    part_key = jax.random.fold_in(base_key, part)
    key_w, key_m, key_g = jax.random.split(part_key, 3)
    shared_key = jax.random.key(seed + 4241)
    key_lr, key_mu, key_wd = jax.random.split(shared_key, 3)
    weight = 0.25 * jax.random.normal(key_w, (MATRICES, ROW_DIM, COL_DIM), jnp.float32)
    momentum = low_rank_draw(key_m, 8)
    gradient = low_rank_draw(key_g, 8).astype(jnp.bfloat16)
    learn_rate = jax.random.uniform(key_lr, (), jnp.float32, 0.5, 1.0)
    mom_coef = jax.random.uniform(key_mu, (), jnp.float32, 0.1, 0.95)
    weight_decay = jax.random.uniform(key_wd, (), jnp.float32, 0.2, 0.6)
    return {'weight': weight, 'momentum': momentum, 'gradient': gradient, 'learn_rate': learn_rate, 'mom_coef': mom_coef, 'weight_decay': weight_decay}


def newton_schulz(x_iter):
    for step_idx in range(NS_STEPS):
        gram_mat = jnp.dot(x_iter.T, x_iter, preferred_element_type=jnp.float32).astype(jnp.bfloat16)
        gram_sq = jnp.dot(gram_mat, gram_mat, preferred_element_type=jnp.float32).astype(jnp.bfloat16)
        poly_mat = (COEF_B * gram_mat.astype(jnp.float32) + COEF_C * gram_sq.astype(jnp.float32)).astype(jnp.bfloat16)
        update = jnp.dot(x_iter, poly_mat.T, preferred_element_type=jnp.float32)
        x_iter = (COEF_A * x_iter.astype(jnp.float32) + update).astype(jnp.bfloat16)
    return x_iter


def reference(weight, momentum, gradient, learn_rate, mom_coef, weight_decay):
    def one_matrix(blocks):
        w_mat, m_mat, g_mat = blocks
        grad_full = g_mat.astype(jnp.float32)
        mom_new = mom_coef * m_mat + grad_full
        nesterov = grad_full + mom_coef * mom_new
        norm_val = jnp.sqrt(jnp.sum(nesterov * nesterov))
        x_iter = (nesterov / (norm_val + NORM_EPS)).astype(jnp.bfloat16)
        x_iter = newton_schulz(x_iter)
        step_scale = learn_rate * 0.2 * math.sqrt(ROW_DIM)
        w_new = (1.0 - learn_rate * weight_decay) * w_mat - step_scale * x_iter.astype(jnp.float32)
        return w_new, mom_new
    new_weight, new_momentum = lax.map(one_matrix, (weight, momentum, gradient))
    return (new_weight, new_momentum)
```

```python
import functools
import math

import jax
import jax.numpy as jnp
from jax import lax
from jax.experimental import pallas as pl
from jax.experimental.pallas import tpu as pltpu
from jax.sharding import PartitionSpec as P

NS_STEPS = 5
COEF_A = 3.4445
COEF_B = -4.7750
COEF_C = 2.0315
NORM_EPS = 1e-7

MESH = pl.DeviceIdType.MESH
F32 = jnp.float32
BF16 = jnp.bfloat16

BLK = 512
VMEM_LIMIT = 64 * 1024 * 1024 - 65536


def here():
    fsdp = lax.axis_index('fsdp')
    tp = lax.axis_index('tp')
    return fsdp, tp, tp // 2, tp % 2


def tri_index(step, num_blk):
    step = jnp.asarray(step, jnp.int32)
    row = jnp.int32(0)
    start = jnp.int32(0)
    first = 0
    for blk in range(1, num_blk):
        first += num_blk - blk + 1
        past = (step >= first).astype(jnp.int32)
        row = row + past
        start = start + past * (num_blk - blk + 1)
    return row, step - start + row


def dot_tn(lhs, rhs):
    return lax.dot_general(lhs, rhs, (((0,), (0,)), ((), ())), preferred_element_type=F32)


def spread_kernel(rows, cols, x_ref, out_ref, stage_ref, send_sem, recv_sem, loc_sem):
    fsdp, tp, chip, core = here()
    barrier = pltpu.get_barrier_semaphore()
    targets = []
    for off in range(8):
        far_f = (fsdp + off // 4) % 2
        far_x = (chip + (off // 2) % 2) % 2
        far_c = (core + off % 2) % 2
        targets.append((far_f, far_x, far_c))
    for off in range(1, 8):
        far_f, far_x, far_c = targets[off]
        pl.semaphore_signal(barrier, inc=1, device_id={'fsdp': far_f, 'tp': 2 * far_x + far_c}, device_id_type=MESH)
    pl.semaphore_wait(barrier, 7)

    def piece(off):
        far_f, far_x, far_c = targets[off]
        mat = (far_f + far_x) % 2
        src = x_ref.at[mat, pl.ds(pl.multiple_of(far_c * rows, rows), rows), :]
        dst = out_ref.at[pl.ds(pl.multiple_of(fsdp * rows, rows), rows), pl.ds(pl.multiple_of(tp * cols, cols), cols)]
        return src, dst

    copies = []
    for off in (6, 7, 2, 3, 4, 5, 1):
        far_f, far_x, far_c = targets[off]
        src, dst = piece(off)
        copy = pltpu.make_async_remote_copy(
            src_ref=src, dst_ref=dst, send_sem=send_sem.at[off], recv_sem=recv_sem.at[off],
            device_id={'fsdp': far_f, 'tp': 2 * far_x + far_c}, device_id_type=MESH)
        copy.start()
        copies.append(copy)
    src, dst = piece(0)
    to_vmem = pltpu.make_async_copy(src, stage_ref, loc_sem.at[0])
    to_vmem.start()
    to_vmem.wait()
    to_hbm = pltpu.make_async_copy(stage_ref, dst, loc_sem.at[1])
    to_hbm.start()
    to_hbm.wait()
    for copy in copies:
        copy.wait()


def spread(x_loc):
    _, rows, cols = x_loc.shape
    rows = rows // 2
    return pl.pallas_call(
        functools.partial(spread_kernel, rows, cols),
        out_shape=jax.ShapeDtypeStruct((2 * rows, 4 * cols), BF16),
        in_specs=[pl.BlockSpec(memory_space=pl.ANY)],
        out_specs=pl.BlockSpec(memory_space=pl.ANY),
        scratch_shapes=[
            pltpu.VMEM((rows, cols), BF16),
            pltpu.SemaphoreType.DMA((8,)),
            pltpu.SemaphoreType.DMA((8,)),
            pltpu.SemaphoreType.DMA((2,)),
        ],
        compiler_params=pltpu.CompilerParams(collective_id=0, has_side_effects=True, vmem_limit_bytes=VMEM_LIMIT),
        name='spread',
    )(x_loc)


def poly_kernel(num_blk, xi_ref, xj_ref, b_ref, a_ref, part_ref, got_ref, stage_ref,
                psend, precv, asend, arecv, bloc, bsend, brecv):
    total = num_blk * (num_blk + 1) // 2
    step = pl.program_id(0)
    _, tp, chip, core = here()
    peer = {'tp': 2 * chip + 1 - core}

    @pl.when(step == 0)
    def _():
        barrier = pltpu.get_barrier_semaphore()
        pl.semaphore_signal(barrier, inc=1, device_id=peer, device_id_type=MESH)
        pl.semaphore_wait(barrier, 1)

    def rows_of(blk):
        return pl.ds(pl.multiple_of(blk * BLK, BLK), BLK)

    def part_copy(num):
        return pltpu.make_async_remote_copy(
            src_ref=part_ref.at[num % 2], dst_ref=got_ref.at[num // 2], send_sem=psend.at[num], recv_sem=precv.at[num],
            device_id=peer, device_id_type=MESH)

    def a_copy(num, flip):
        row, col = tri_index(num, num_blk)
        if flip:
            row, col = col, row
        ref = a_ref.at[col, rows_of(row), :]
        return pltpu.make_async_remote_copy(
            src_ref=ref, dst_ref=ref, send_sem=asend.at[flip, num], recv_sem=arecv.at[flip, num],
            device_id=peer, device_id_type=MESH)

    def finish(num):
        row, col = tri_index(num, num_blk)
        part_copy(num).wait_recv()
        val = part_ref[num % 2] + got_ref[num // 2]
        a_ref[col, rows_of(row), :] = val.astype(BF16)
        a_copy(num, 0).start()

        @pl.when(row != col)
        def _():
            a_ref[row, rows_of(col), :] = val.T.astype(BF16)
            a_copy(num, 1).start()

    part_ref[step % 2] = dot_tn(xi_ref[...], xj_ref[...])
    mine = (step + core) % 2 == 0
    theirs = (step + core) % 2 == 1

    @pl.when(theirs)
    def _():
        part_copy(step).start()

    @pl.when(jnp.logical_and(step >= 1, theirs))
    def _():
        finish(step - 1)

    @pl.when(jnp.logical_and(step >= 1, mine))
    def _():
        part_copy(step - 1).wait_send()

    @pl.when(step == total - 1)
    def _():
        @pl.when(mine)
        def _():
            finish(total - 1)

        @pl.when(theirs)
        def _():
            part_copy(total - 1).wait_send()

        num_mine = (total + 1) // 2 - (total % 2) * core
        num_theirs = total // 2 + (total % 2) * core

        def wait_sent(k, _):
            num = 2 * k + core
            row, col = tri_index(num, num_blk)
            a_copy(num, 0).wait_send()

            @pl.when(row != col)
            def _():
                a_copy(num, 1).wait_send()
            return 0

        def wait_got(k, _):
            num = 2 * k + 1 - core
            row, col = tri_index(num, num_blk)
            a_copy(num, 0).wait_recv()

            @pl.when(row != col)
            def _():
                a_copy(num, 1).wait_recv()
            return 0

        lax.fori_loop(0, num_theirs, wait_got, 0)
        lax.fori_loop(0, num_mine, wait_sent, 0)

        def b_copies(num, flip):
            slot = (num // 2) % 2
            row, col = tri_index(num, num_blk)
            if flip:
                row, col = col, row
            src = stage_ref.at[slot, flip]
            dst = b_ref.at[rows_of(row), rows_of(col)]
            local = pltpu.make_async_copy(src, dst, bloc.at[flip, num])
            remote = pltpu.make_async_remote_copy(
                src_ref=src, dst_ref=dst, send_sem=bsend.at[flip, num], recv_sem=brecv.at[flip, num],
                device_id=peer, device_id_type=MESH)
            return local, remote

        def b_drain(num):
            row, col = tri_index(num, num_blk)
            local, remote = b_copies(num, 0)
            local.wait()
            remote.wait_send()

            @pl.when(row != col)
            def _():
                local, remote = b_copies(num, 1)
                local.wait()
                remote.wait_send()

        def square(k, _):
            num = 2 * k + core
            row, col = tri_index(num, num_blk)
            slot = k % 2

            @pl.when(k >= 2)
            def _():
                b_drain(num - 4)

            gram_sq = dot_tn(a_ref[row], a_ref[col]).astype(BF16)
            gram = a_ref[col, rows_of(row), :]
            poly = COEF_B * gram.astype(F32) + COEF_C * gram_sq.astype(F32)
            stage_ref[slot, 0] = poly.astype(BF16)
            local, remote = b_copies(num, 0)
            remote.start()
            local.start()

            @pl.when(row != col)
            def _():
                stage_ref[slot, 1] = poly.T.astype(BF16)
                local, remote = b_copies(num, 1)
                remote.start()
                local.start()
            return 0

        lax.fori_loop(0, num_mine, square, 0)
        b_drain(2 * (num_mine - 2) + core)
        b_drain(2 * (num_mine - 1) + core)

        def wait_b(k, _):
            num = 2 * k + 1 - core
            row, col = tri_index(num, num_blk)
            b_copies(num, 0)[1].wait_recv()

            @pl.when(row != col)
            def _():
                b_copies(num, 1)[1].wait_recv()
            return 0

        lax.fori_loop(0, num_theirs, wait_b, 0)


def poly(x_mat):
    rows, cols = x_mat.shape
    num_blk = cols // BLK
    total = num_blk * (num_blk + 1) // 2
    half = (total + 1) // 2
    dma = pltpu.SemaphoreType.DMA
    return pl.pallas_call(
        functools.partial(poly_kernel, num_blk),
        grid=(total,),
        out_shape=jax.ShapeDtypeStruct((cols, cols), BF16),
        in_specs=[
            pl.BlockSpec((rows, BLK), lambda s: (0, tri_index(s, num_blk)[0])),
            pl.BlockSpec((rows, BLK), lambda s: (0, tri_index(s, num_blk)[1])),
        ],
        out_specs=pl.BlockSpec(memory_space=pl.ANY),
        scratch_shapes=[
            pltpu.VMEM((num_blk, cols, BLK), BF16),
            pltpu.VMEM((2, BLK, BLK), F32),
            pltpu.VMEM((half, BLK, BLK), F32),
            pltpu.VMEM((2, 2, BLK, BLK), BF16),
            dma((total,)), dma((total,)),
            dma((2, total)), dma((2, total)),
            dma((2, total)), dma((2, total)), dma((2, total)),
        ],
        compiler_params=pltpu.CompilerParams(
            collective_id=1, has_side_effects=True, vmem_limit_bytes=VMEM_LIMIT, dimension_semantics=('arbitrary',)),
        name='poly',
    )(x_mat, x_mat)


def update_kernel(tile, x_ref, b_ref, out_ref):
    blk = pl.program_id(0)
    upd = jnp.dot(x_ref[...], b_ref[...], preferred_element_type=F32)
    x_old = x_ref[:, pl.ds(pl.multiple_of(blk * tile, tile), tile)]
    out_ref[...] = (COEF_A * x_old.astype(F32) + upd).astype(BF16)


def update(x_mat, b_mat, row_tile=512, col_tile=1024):
    rows, cols = x_mat.shape
    return pl.pallas_call(
        functools.partial(update_kernel, col_tile),
        grid=(cols // col_tile, rows // row_tile),
        out_shape=jax.ShapeDtypeStruct((rows, cols), BF16),
        in_specs=[
            pl.BlockSpec((row_tile, cols), lambda j, i: (i, 0)),
            pl.BlockSpec((cols, col_tile), lambda j, i: (0, j)),
        ],
        out_specs=pl.BlockSpec((row_tile, col_tile), lambda j, i: (i, j)),
        compiler_params=pltpu.CompilerParams(
            vmem_limit_bytes=VMEM_LIMIT, dimension_semantics=('arbitrary', 'arbitrary')),
        name='update',
    )(x_mat, b_mat)


def last_kernel(tile, tab_ref, x_ref, b_ref, out_ref):
    blk = tab_ref[1, pl.program_id(0)]
    upd = jnp.dot(x_ref[...], b_ref[...], preferred_element_type=F32)
    x_old = x_ref[:, pl.ds(pl.multiple_of(blk * tile, tile), tile)]
    out_ref[0] = (COEF_A * x_old.astype(F32) + upd).astype(BF16)


def last_update(x_mat, b_mat, table, row_tile=512):
    rows, cols = x_mat.shape
    half, tile = rows // 2, cols // 4
    per = half // row_tile
    return pl.pallas_call(
        functools.partial(last_kernel, tile),
        grid_spec=pltpu.PrefetchScalarGridSpec(
            num_scalar_prefetch=1,
            grid=(4, per),
            in_specs=[
                pl.BlockSpec((row_tile, cols), lambda p, i, tab: (tab[0, p] * per + i, 0)),
                pl.BlockSpec((cols, tile), lambda p, i, tab: (0, tab[1, p])),
            ],
            out_specs=pl.BlockSpec((1, row_tile, tile), lambda p, i, tab: (p, i, 0)),
        ),
        out_shape=jax.ShapeDtypeStruct((4, half, tile), BF16),
        compiler_params=pltpu.CompilerParams(
            vmem_limit_bytes=VMEM_LIMIT, dimension_semantics=('arbitrary', 'arbitrary')),
        name='last_update',
    )(table, x_mat, b_mat)


def collect_kernel(rows, in_ref, out_ref, stage_ref, send_sem, recv_sem, loc_sem):
    fsdp, tp, chip, core = here()
    mat = (fsdp + chip) % 2
    peers = [
        {'fsdp': fsdp, 'tp': 2 * (1 - chip)},
        {'fsdp': 1 - fsdp, 'tp': 2 * chip + 1},
        {'fsdp': fsdp, 'tp': 2 * chip + 1 - core},
    ]
    far = [{'fsdp': fsdp * (1 - core) + (1 - fsdp) * core, 'tp': 2 * (chip * core + (1 - chip) * (1 - core)) + k} for k in (0, 1)]
    barrier = pltpu.get_barrier_semaphore()
    for dev in far + [peers[2]]:
        pl.semaphore_signal(barrier, inc=1, device_id=dev, device_id_type=MESH)
    pl.semaphore_wait(barrier, 3)

    def dst(which):
        return out_ref.at[which, pl.ds(pl.multiple_of(core * rows, rows), rows), :]

    def copy(num):
        return pltpu.make_async_remote_copy(
            src_ref=in_ref.at[num], dst_ref=dst(mat), send_sem=send_sem.at[num],
            recv_sem=recv_sem.at[core if num < 2 else 2], device_id=peers[num], device_id_type=MESH)

    copies = [copy(num) for num in range(3)]
    for item in copies:
        item.start()
    to_vmem = pltpu.make_async_copy(in_ref.at[3], stage_ref, loc_sem.at[0])
    to_vmem.start()
    to_vmem.wait()
    to_hbm = pltpu.make_async_copy(stage_ref, dst(mat), loc_sem.at[1])
    to_hbm.start()
    to_hbm.wait()
    for item in copies:
        item.wait_send()
    for k in (0, 1):
        pltpu.make_async_remote_copy(
            src_ref=in_ref.at[0], dst_ref=out_ref.at[1 - mat, pl.ds(k * rows, rows), :], send_sem=send_sem.at[0],
            recv_sem=recv_sem.at[k], device_id=far[k], device_id_type=MESH).wait_recv()
    pltpu.make_async_remote_copy(
        src_ref=in_ref.at[2], dst_ref=out_ref.at[mat, pl.ds(pl.multiple_of((1 - core) * rows, rows), rows), :],
        send_sem=send_sem.at[2], recv_sem=recv_sem.at[2], device_id=peers[2], device_id_type=MESH).wait_recv()


def collect(pieces):
    _, rows, cols = pieces.shape
    dma = pltpu.SemaphoreType.DMA
    return pl.pallas_call(
        functools.partial(collect_kernel, rows),
        out_shape=jax.ShapeDtypeStruct((2, 2 * rows, cols), BF16),
        in_specs=[pl.BlockSpec(memory_space=pl.ANY)],
        out_specs=pl.BlockSpec(memory_space=pl.ANY),
        scratch_shapes=[pltpu.VMEM((rows, cols), BF16), dma((3,)), dma((3,)), dma((2,))],
        compiler_params=pltpu.CompilerParams(collective_id=2, has_side_effects=True, vmem_limit_bytes=VMEM_LIMIT),
        name='collect',
    )(pieces)


def solution(mesh):
    fsdp_size = mesh.shape['fsdp']
    mat_spec = P('stage', 'fsdp', 'tp')
    scalar_spec = P()

    def local_step(weight, momentum, gradient, learn_rate, mom_coef, weight_decay):
        row_dim = weight.shape[1] * fsdp_size
        fsdp, tp, chip, core = here()
        grad_full = gradient.astype(F32)
        mom_new = mom_coef * momentum + grad_full
        nesterov = grad_full + mom_coef * mom_new
        sq_sum = lax.psum(jnp.sum(nesterov * nesterov, axis=(1, 2)), ('fsdp', 'tp'))
        norm_val = jnp.sqrt(sq_sum)[:, None, None]
        x_loc = (nesterov / (norm_val + NORM_EPS)).astype(BF16)
        x_mat = spread(x_loc)
        for _ in range(NS_STEPS - 1):
            x_mat = update(x_mat, poly(x_mat))
        row_half = jnp.stack([fsdp, 1 - fsdp, fsdp, fsdp])
        col_quarter = jnp.stack([2 * (1 - chip), 2 * chip + 1, 2 * chip + 1 - core, 2 * chip + core])
        table = jnp.stack([row_half, col_quarter]).astype(jnp.int32)
        x_fin = collect(last_update(x_mat, poly(x_mat), table))
        step_scale = learn_rate * 0.2 * math.sqrt(row_dim)
        new_weight = (1.0 - learn_rate * weight_decay) * weight - step_scale * x_fin.astype(F32)
        return new_weight, mom_new

    return jax.shard_map(local_step, mesh=mesh, in_specs=(mat_spec,) * 3 + (scalar_spec,) * 3, out_specs=(mat_spec, mat_spec), check_vma=False)
```

```python
import functools
import math

import jax
import jax.numpy as jnp
from jax import lax
from jax.experimental import pallas as pl
from jax.experimental.pallas import tpu as pltpu
from jax.sharding import PartitionSpec as P


NS_STEPS = 5
COEF_A = 3.4445
COEF_B = -4.7750
COEF_C = 2.0315
NORM_EPS = 1e-7


MESH = pl.DeviceIdType.MESH
F32 = jnp.float32
BF16 = jnp.bfloat16

BLK = 512
VMEM_LIMIT = 64 * 1024 * 1024 - 65536


def here():
    fsdp = lax.axis_index('fsdp')
    tp = lax.axis_index('tp')
    return fsdp, tp, tp // 2, tp % 2


def tri_index(step, num_blk):
    step = jnp.asarray(step, jnp.int32)
    row = jnp.int32(0)
    start = jnp.int32(0)
    first = 0
    for blk in range(1, num_blk):
        first += num_blk - blk + 1
        past = (step >= first).astype(jnp.int32)
        row = row + past
        start = start + past * (num_blk - blk + 1)
    return row, step - start + row


def dot_tn(lhs, rhs):
    return lax.dot_general(lhs, rhs, (((0,), (0,)), ((), ())), preferred_element_type=F32)


CHUNK = 512


def spread_kernel(rows, cols, mu_ref, sq_ref, m_ref, g_ref, out_ref, all_ref, m_buf, g_buf, x_buf,
                  load_sem, nsend, nrecv, send_sem, recv_sem):
    fsdp, tp, chip, core = here()
    me = 4 * fsdp + tp
    per = rows // CHUNK
    steps = 4 * per
    chips = ((0, 1), (1, 0), (1, 1), (0, 0))

    def device(hop, flip):
        far_f = (fsdp + chips[hop][0]) % 2
        far_x = (chip + chips[hop][1]) % 2
        far_c = (core + flip) % 2
        return far_f, 2 * far_x + far_c

    others = [(hop, flip) for hop in range(4) for flip in range(2) if (hop, flip) != (3, 0)]

    def m_load(mat, first, slot):
        return pltpu.make_async_copy(m_ref.at[mat, pl.ds(first, CHUNK), :], m_buf.at[slot], load_sem.at[0, slot])

    def g_load(mat, first, slot):
        return pltpu.make_async_copy(g_ref.at[mat, pl.ds(first, CHUNK), :], g_buf.at[slot], load_sem.at[1, slot])

    def where(step):
        near = step // (2 * per)
        flip = (step // per) % 2
        quarter = step % per
        mat = (fsdp + chip + 1 - near) % 2
        far_c = (core + flip) % 2
        first = pl.multiple_of(far_c * rows + quarter * CHUNK, CHUNK)
        return near, flip, quarter, mat, first

    def load(step, slot):
        _, _, _, mat, first = where(step)
        m_load(mat, first, slot).start()
        g_load(mat, first, slot).start()

    load(0, 0)
    barrier = pltpu.get_barrier_semaphore()
    for hop, flip in others:
        far_f, far_t = device(hop, flip)
        pl.semaphore_signal(barrier, inc=1, device_id={'fsdp': far_f, 'tp': far_t}, device_id_type=MESH)
    pl.semaphore_wait(barrier, 7)

    all_ref[me] = sq_ref[...]
    norm_copies = []
    for num, (hop, flip) in enumerate(others):
        far_f, far_t = device(hop, flip)
        copy = pltpu.make_async_remote_copy(
            src_ref=sq_ref, dst_ref=all_ref.at[me], send_sem=nsend.at[num], recv_sem=nrecv.at[num],
            device_id={'fsdp': far_f, 'tp': far_t}, device_id_type=MESH)
        copy.start()
        norm_copies.append(copy)
    for copy in norm_copies:
        copy.wait()
    total = all_ref[0]
    for dev in range(1, 8):
        total = total + all_ref[dev]
    norm = jnp.sqrt(total) + NORM_EPS
    mu = mu_ref[0]

    def x_copy(hop, flip, step, quarter):
        far_f, _ = device(hop, 0)
        far_x = (chip + chips[hop][1]) % 2
        far_t = 2 * far_x + (core + flip) % 2
        dst = out_ref.at[pl.ds(pl.multiple_of(fsdp * rows + quarter * CHUNK, CHUNK), CHUNK),
                         pl.ds(pl.multiple_of(tp * cols, cols), cols)]
        return pltpu.make_async_remote_copy(
            src_ref=x_buf.at[step], dst_ref=dst, send_sem=send_sem.at[hop, flip, quarter],
            recv_sem=recv_sem.at[hop, flip, quarter], device_id={'fsdp': far_f, 'tp': far_t}, device_id_type=MESH)

    def own_copy(step, quarter):
        dst = out_ref.at[pl.ds(pl.multiple_of(fsdp * rows + quarter * CHUNK, CHUNK), CHUNK),
                         pl.ds(pl.multiple_of(tp * cols, cols), cols)]
        return pltpu.make_async_copy(x_buf.at[step], dst, send_sem.at[3, 0, quarter])

    def make(step, _):
        near, flip, quarter, mat, first = where(step)
        slot = step % 2
        m_load(mat, first, slot).wait()
        g_load(mat, first, slot).wait()

        @pl.when(step + 1 < steps)
        def _():
            load(step + 1, 1 - slot)

        grad = g_buf[slot].astype(F32)
        nesterov = grad + mu * (mu * m_buf[slot] + grad)
        scale = jnp.where(mat == 0, norm[0:1, 0:1], norm[1:2, 0:1])
        x_buf[step] = (nesterov / scale).astype(BF16)

        @pl.when(near == 0)
        def _():
            x_copy(0, flip, step, quarter).start()
            x_copy(1, flip, step, quarter).start()

        @pl.when(near == 1)
        def _():
            x_copy(2, flip, step, quarter).start()

            @pl.when(flip == 1)
            def _():
                x_copy(3, flip, step, quarter).start()

            @pl.when(flip == 0)
            def _():
                own_copy(step, quarter).start()

        return 0

    lax.fori_loop(0, steps, make, 0)
    for quarter in range(per):
        own_copy(2 * per + quarter, quarter).wait()
        for hop, flip in others:
            step = (hop // 2) * 2 * per + flip * per + quarter
            x_copy(hop, flip, step, quarter).wait()


def spread(mu, sq_sum, momentum, gradient):
    mats, rows, cols = momentum.shape
    rows = rows // 2
    dma = pltpu.SemaphoreType.DMA
    per = rows // CHUNK
    sq_tile = jnp.zeros((8, 128), F32).at[:mats].set(sq_sum[:, None])
    return pl.pallas_call(
        functools.partial(spread_kernel, rows, cols),
        out_shape=jax.ShapeDtypeStruct((2 * rows, 4 * cols), BF16),
        in_specs=[
            pl.BlockSpec(memory_space=pltpu.SMEM),
            pl.BlockSpec(memory_space=pltpu.VMEM),
            pl.BlockSpec(memory_space=pl.ANY),
            pl.BlockSpec(memory_space=pl.ANY),
        ],
        out_specs=pl.BlockSpec(memory_space=pl.ANY),
        scratch_shapes=[
            pltpu.VMEM((8, 8, 128), F32),
            pltpu.VMEM((2, CHUNK, cols), F32),
            pltpu.VMEM((2, CHUNK, cols), BF16),
            pltpu.VMEM((4 * per, CHUNK, cols), BF16),
            dma((2, 2)), dma((7,)), dma((7,)),
            dma((4, 2, per)), dma((4, 2, per)),
        ],
        compiler_params=pltpu.CompilerParams(collective_id=0, has_side_effects=True, vmem_limit_bytes=VMEM_LIMIT),
        name='spread',
    )(mu.reshape(1), sq_tile, momentum, gradient)


def poly_kernel(num_blk, x_hbm, b_ref, x_ref, a_ref, part_ref, got_ref, stage_ref,
                xsem, psend, precv, asend, arecv, bloc, bsend, brecv):
    total = num_blk * (num_blk + 1) // 2
    _, _, chip, core = here()
    peer = {'tp': 2 * chip + 1 - core}

    def x_load(blk):
        return pltpu.make_async_copy(
            x_hbm.at[:, pl.ds(pl.multiple_of(blk * BLK, BLK), BLK)], x_ref.at[blk], xsem.at[blk])

    for blk in range(num_blk):
        x_load(blk).start()
    barrier = pltpu.get_barrier_semaphore()
    pl.semaphore_signal(barrier, inc=1, device_id=peer, device_id_type=MESH)
    pl.semaphore_wait(barrier, 1)

    def rows_of(blk):
        return pl.ds(pl.multiple_of(blk * BLK, BLK), BLK)

    def part_copy(num):
        return pltpu.make_async_remote_copy(
            src_ref=part_ref.at[num % 2], dst_ref=got_ref.at[num // 2], send_sem=psend.at[num], recv_sem=precv.at[num],
            device_id=peer, device_id_type=MESH)

    def a_copy(num, flip):
        row, col = tri_index(num, num_blk)
        if flip:
            row, col = col, row
        ref = a_ref.at[col, rows_of(row), :]
        return pltpu.make_async_remote_copy(
            src_ref=ref, dst_ref=ref, send_sem=asend.at[flip, num], recv_sem=arecv.at[flip, num],
            device_id=peer, device_id_type=MESH)

    def finish(num):
        row, col = tri_index(num, num_blk)
        part_copy(num).wait_recv()
        val = part_ref[num % 2] + got_ref[num // 2]
        a_ref[col, rows_of(row), :] = val.astype(BF16)
        a_copy(num, 0).start()

        @pl.when(row != col)
        def _():
            a_ref[row, rows_of(col), :] = val.T.astype(BF16)
            a_copy(num, 1).start()

    def gram(step, _):
        row, col = tri_index(step, num_blk)

        @pl.when(row == 0)
        def _():
            x_load(col).wait()

        part_ref[step % 2] = dot_tn(x_ref[row], x_ref[col])
        mine = (step + core) % 2 == 0
        theirs = (step + core) % 2 == 1

        @pl.when(theirs)
        def _():
            part_copy(step).start()

        @pl.when(jnp.logical_and(step >= 1, theirs))
        def _():
            finish(step - 1)

        @pl.when(jnp.logical_and(step >= 1, mine))
        def _():
            part_copy(step - 1).wait_send()

        return 0

    lax.fori_loop(0, total, gram, 0)
    last_mine = (total - 1 + core) % 2 == 0
    last_theirs = (total - 1 + core) % 2 == 1

    @pl.when(last_mine)
    def _():
        finish(total - 1)

    @pl.when(last_theirs)
    def _():
        part_copy(total - 1).wait_send()

    num_mine = (total + 1) // 2 - (total % 2) * core
    num_theirs = total // 2 + (total % 2) * core

    def wait_sent(k, _):
        num = 2 * k + core
        row, col = tri_index(num, num_blk)
        a_copy(num, 0).wait_send()

        @pl.when(row != col)
        def _():
            a_copy(num, 1).wait_send()

        return 0

    def wait_got(k, _):
        num = 2 * k + 1 - core
        row, col = tri_index(num, num_blk)
        a_copy(num, 0).wait_recv()

        @pl.when(row != col)
        def _():
            a_copy(num, 1).wait_recv()

        return 0

    lax.fori_loop(0, num_theirs, wait_got, 0)
    lax.fori_loop(0, num_mine, wait_sent, 0)

    def b_copies(num, flip):
        slot = (num // 2) % 2
        row, col = tri_index(num, num_blk)
        if flip:
            row, col = col, row
        src = stage_ref.at[slot, flip]
        dst = b_ref.at[rows_of(row), rows_of(col)]
        local = pltpu.make_async_copy(src, dst, bloc.at[flip, num])
        remote = pltpu.make_async_remote_copy(
            src_ref=src, dst_ref=dst, send_sem=bsend.at[flip, num], recv_sem=brecv.at[flip, num],
            device_id=peer, device_id_type=MESH)
        return local, remote

    def b_drain(num):
        row, col = tri_index(num, num_blk)
        local, remote = b_copies(num, 0)
        local.wait()
        remote.wait_send()

        @pl.when(row != col)
        def _():
            local, remote = b_copies(num, 1)
            local.wait()
            remote.wait_send()

    def square(k, _):
        num = 2 * k + core
        row, col = tri_index(num, num_blk)
        slot = k % 2

        @pl.when(k >= 2)
        def _():
            b_drain(num - 4)

        gram_sq = dot_tn(a_ref[row], a_ref[col]).astype(BF16)
        gram = a_ref[col, rows_of(row), :]
        poly = COEF_B * gram.astype(F32) + COEF_C * gram_sq.astype(F32)
        stage_ref[slot, 0] = poly.astype(BF16)
        local, remote = b_copies(num, 0)
        remote.start()
        local.start()

        @pl.when(row != col)
        def _():
            stage_ref[slot, 1] = poly.T.astype(BF16)
            local, remote = b_copies(num, 1)
            remote.start()
            local.start()

        return 0

    lax.fori_loop(0, num_mine, square, 0)
    b_drain(2 * (num_mine - 2) + core)
    b_drain(2 * (num_mine - 1) + core)

    def wait_b(k, _):
        num = 2 * k + 1 - core
        row, col = tri_index(num, num_blk)
        b_copies(num, 0)[1].wait_recv()

        @pl.when(row != col)
        def _():
            b_copies(num, 1)[1].wait_recv()

        return 0

    lax.fori_loop(0, num_theirs, wait_b, 0)


def poly(x_mat):
    rows, cols = x_mat.shape
    num_blk = cols // BLK
    total = num_blk * (num_blk + 1) // 2
    half = (total + 1) // 2
    dma = pltpu.SemaphoreType.DMA
    return pl.pallas_call(
        functools.partial(poly_kernel, num_blk),
        out_shape=jax.ShapeDtypeStruct((cols, cols), BF16),
        in_specs=[pl.BlockSpec(memory_space=pl.ANY)],
        out_specs=pl.BlockSpec(memory_space=pl.ANY),
        scratch_shapes=[
            pltpu.VMEM((num_blk, rows, BLK), BF16),
            pltpu.VMEM((num_blk, cols, BLK), BF16),
            pltpu.VMEM((2, BLK, BLK), F32),
            pltpu.VMEM((half, BLK, BLK), F32),
            pltpu.VMEM((2, 2, BLK, BLK), BF16),
            dma((num_blk,)), dma((total,)), dma((total,)),
            dma((2, total)), dma((2, total)),
            dma((2, total)), dma((2, total)), dma((2, total)),
        ],
        compiler_params=pltpu.CompilerParams(
            collective_id=1, has_side_effects=True, vmem_limit_bytes=VMEM_LIMIT),
        name='poly',
    )(x_mat)


def update_kernel(tile, x_ref, b_ref, out_ref):
    blk = pl.program_id(0)
    upd = jnp.dot(x_ref[...], b_ref[...], preferred_element_type=F32)
    x_old = x_ref[:, pl.ds(pl.multiple_of(blk * tile, tile), tile)]
    out_ref[...] = (COEF_A * x_old.astype(F32) + upd).astype(BF16)


def update(x_mat, b_mat, row_tile=1024, col_tile=1024):
    rows, cols = x_mat.shape
    return pl.pallas_call(
        functools.partial(update_kernel, col_tile),
        grid=(cols // col_tile, rows // row_tile),
        out_shape=jax.ShapeDtypeStruct((rows, cols), BF16),
        in_specs=[
            pl.BlockSpec((row_tile, cols), lambda j, i: (i, 0)),
            pl.BlockSpec((cols, col_tile), lambda j, i: (0, j)),
        ],
        out_specs=pl.BlockSpec((row_tile, col_tile), lambda j, i: (i, j)),
        compiler_params=pltpu.CompilerParams(
            vmem_limit_bytes=VMEM_LIMIT, dimension_semantics=('arbitrary', 'arbitrary')),
        name='update',
    )(x_mat, b_mat)


def pair_kernel(tile, base, tab_ref, x_ref, b_ref, out0_ref, out1_ref):
    which = pl.program_id(0)
    blk = tab_ref[1, base + which]
    upd = jnp.dot(x_ref[...], b_ref[...], preferred_element_type=F32)
    x_old = x_ref[:, pl.ds(pl.multiple_of(blk * tile, tile), tile)]
    val = (COEF_A * x_old.astype(F32) + upd).astype(BF16)

    @pl.when(which == 0)
    def _():
        out0_ref[...] = val

    @pl.when(which == 1)
    def _():
        out1_ref[...] = val


def last_pieces(x_mat, b_mat, table, base, piece_rows, row_tile=1024):
    _, cols = x_mat.shape
    tile = cols // 4
    last = piece_rows // row_tile - 1
    return pl.pallas_call(
        functools.partial(pair_kernel, tile, base),
        grid_spec=pltpu.PrefetchScalarGridSpec(
            num_scalar_prefetch=1,
            grid=(2, last + 1),
            in_specs=[
                pl.BlockSpec((row_tile, cols), lambda p, i, tab: (tab[0, base + p] + i, 0)),
                pl.BlockSpec((cols, tile), lambda p, i, tab: (0, tab[1, base + p])),
            ],
            out_specs=[
                pl.BlockSpec((row_tile, tile), lambda p, i, tab: (i * (1 - p) + last * p, 0)),
                pl.BlockSpec((row_tile, tile), lambda p, i, tab: (i * p, 0)),
            ],
        ),
        out_shape=[jax.ShapeDtypeStruct((piece_rows, tile), BF16)] * 2,
        compiler_params=pltpu.CompilerParams(
            vmem_limit_bytes=VMEM_LIMIT, dimension_semantics=('arbitrary', 'arbitrary')),
        cost_estimate=pl.CostEstimate(
            flops=4 * piece_rows * tile * cols, bytes_accessed=4 * cols * (piece_rows + tile), transcendentals=0),
        name='last_pieces',
    )(table, x_mat, b_mat)


def apply_kernel(tab_ref, scale_ref, w_ref, x_ref, *rest):
    rest[-1][0] = scale_ref[0] * w_ref[0] - scale_ref[1] * x_ref[...].astype(F32)


def apply_piece(weight, x_piece, scales, table, base, so_far, row_tile=512):
    rows, cols = x_piece.shape
    extra = [] if so_far is None else [so_far]
    w_spec = pl.BlockSpec((1, row_tile, cols), lambda i, tab: (tab[0, base], tab[1, base] + i, 0))
    return pl.pallas_call(
        apply_kernel,
        grid_spec=pltpu.PrefetchScalarGridSpec(
            num_scalar_prefetch=1,
            grid=(rows // row_tile,),
            in_specs=[
                pl.BlockSpec(memory_space=pltpu.SMEM),
                w_spec,
                pl.BlockSpec((row_tile, cols), lambda i, tab: (i, 0)),
            ] + [pl.BlockSpec(memory_space=pl.ANY)] * len(extra),
            out_specs=w_spec,
        ),
        out_shape=jax.ShapeDtypeStruct(weight.shape, F32),
        input_output_aliases={4: 0} if extra else {},
        compiler_params=pltpu.CompilerParams(vmem_limit_bytes=VMEM_LIMIT, dimension_semantics=('arbitrary',)),
        cost_estimate=pl.CostEstimate(flops=3 * rows * cols, bytes_accessed=10 * rows * cols, transcendentals=0),
        name='apply_piece',
    )(table, scales, weight, x_piece, *extra)


def solution(mesh):
    fsdp_size = mesh.shape['fsdp']
    mat_spec = P('stage', 'fsdp', 'tp')
    scalar_spec = P()

    def local_step(weight, momentum, gradient, learn_rate, mom_coef, weight_decay):
        row_dim = weight.shape[1] * fsdp_size
        fsdp, _, chip, core = here()
        grad_full = gradient.astype(F32)
        mom_new = mom_coef * momentum + grad_full
        nesterov = grad_full + mom_coef * mom_new
        sq_sum = jnp.sum(nesterov * nesterov, axis=(1, 2))
        sub = row_dim // 4
        half = sub // 2
        mat = (fsdp + chip) % 2
        far = 1 - mat
        r_here, r_far = fsdp * (sub // 1024), (1 - fsdp) * (sub // 1024)
        step = half // 1024
        x_col, y_col = 2 * (1 - chip) + core, 2 * chip + 1 - core
        piece_tab = jnp.stack([
            jnp.stack([r_here, r_far, r_here + step, r_far + step, r_here, r_here]),
            jnp.stack([x_col, y_col, x_col, y_col, y_col, 2 * chip + core]),
        ]).astype(jnp.int32)
        c_here, c_far = core * (sub // 512), (1 - core) * (sub // 512)
        step = half // 512
        apply_tab = jnp.stack([
            jnp.stack([mat, mat, far, far, far, far]),
            jnp.stack([c_here, c_far, c_here, c_far, c_here + step, c_far + step]),
        ]).astype(jnp.int32)
        scales = jnp.stack([1.0 - learn_rate * weight_decay, learn_rate * 0.2 * math.sqrt(row_dim)])
        sq_sum, piece_tab, apply_tab, scales = lax.optimization_barrier((sq_sum, piece_tab, apply_tab, scales))
        x_mat = spread(mom_coef, sq_sum, momentum, gradient)
        for _ in range(NS_STEPS - 1):
            x_mat = update(x_mat, poly(x_mat))
        b_mat = poly(x_mat)

        def permute(piece, kind):
            pairs = []
            for src in range(8):
                f_src, t_src = src // 4, src % 4
                if kind == 'x':
                    dst = f_src * 4 + (t_src + 2) % 4
                elif kind == 'y':
                    dst = (1 - f_src) * 4 + t_src + 1 - 2 * (t_src % 2)
                else:
                    dst = f_src * 4 + t_src + 1 - 2 * (t_src % 2)
                pairs.append((src, dst))
            return lax.ppermute(piece, ('fsdp', 'tp'), pairs)

        moved = []
        tie = b_mat
        for part in range(2):
            to_x, to_y = last_pieces(x_mat, tie, piece_tab, 2 * part, half)
            moved.append(permute(to_x, 'x'))
            moved.append(permute(to_y, 'y'))
            tie, _, _ = lax.optimization_barrier((tie, to_x, to_y))
        near, own = last_pieces(x_mat, tie, piece_tab, 4, sub)
        near = permute(near, 'core')
        new_weight = apply_piece(weight, own, scales, apply_tab, 0, None)
        new_weight = apply_piece(weight, near, scales, apply_tab, 1, new_weight)
        for num, x_piece in enumerate(moved):
            new_weight = apply_piece(weight, x_piece, scales, apply_tab, 2 + num, new_weight)
        return new_weight, mom_new

    return jax.shard_map(local_step, mesh=mesh, in_specs=(mat_spec,) * 3 + (scalar_spec,) * 3, out_specs=(mat_spec, mat_spec), check_vma=False)
```

```python
import functools
import math

import jax
import jax.numpy as jnp
from jax import lax
from jax.experimental import pallas as pl
from jax.experimental.pallas import tpu as pltpu
from jax.sharding import PartitionSpec as P


NS_STEPS = 5
COEF_A = 3.4445
COEF_B = -4.7750
COEF_C = 2.0315
NORM_EPS = 1e-7


MESH = pl.DeviceIdType.MESH
F32 = jnp.float32
BF16 = jnp.bfloat16

BLK = 512
VMEM_LIMIT = 64 * 1024 * 1024 - 65536


def here():
    fsdp = lax.axis_index('fsdp')
    tp = lax.axis_index('tp')
    return fsdp, tp, tp // 2, tp % 2


def tri_index(step, num_blk):
    step = jnp.asarray(step, jnp.int32)
    row = jnp.int32(0)
    start = jnp.int32(0)
    first = 0
    for blk in range(1, num_blk):
        first += num_blk - blk + 1
        past = (step >= first).astype(jnp.int32)
        row = row + past
        start = start + past * (num_blk - blk + 1)
    return row, step - start + row


def dot_tn(lhs, rhs):
    return lax.dot_general(lhs, rhs, (((0,), (0,)), ((), ())), preferred_element_type=F32)


CHUNK = 512


def spread_kernel(rows, cols, mu_ref, sq_ref, m_ref, g_ref, out_ref, all_ref, m_buf, g_buf, x_buf,
                  load_sem, nsend, nrecv, send_sem, recv_sem):
    fsdp, tp, chip, core = here()
    me = 4 * fsdp + tp
    per = rows // CHUNK
    steps = 4 * per
    chips = ((0, 1), (1, 0), (1, 1), (0, 0))

    def device(hop, flip):
        far_f = (fsdp + chips[hop][0]) % 2
        far_x = (chip + chips[hop][1]) % 2
        far_c = (core + flip) % 2
        return far_f, 2 * far_x + far_c

    others = [(hop, flip) for hop in range(4) for flip in range(2) if (hop, flip) != (3, 0)]

    def m_load(mat, first, slot):
        return pltpu.make_async_copy(m_ref.at[mat, pl.ds(first, CHUNK), :], m_buf.at[slot], load_sem.at[0, slot])

    def g_load(mat, first, slot):
        return pltpu.make_async_copy(g_ref.at[mat, pl.ds(first, CHUNK), :], g_buf.at[slot], load_sem.at[1, slot])

    def where(step):
        near = step // (2 * per)
        flip = (step // per) % 2
        quarter = step % per
        mat = (fsdp + chip + 1 - near) % 2
        far_c = (core + flip) % 2
        first = pl.multiple_of(far_c * rows + quarter * CHUNK, CHUNK)
        return near, flip, quarter, mat, first

    def load(step, slot):
        _, _, _, mat, first = where(step)
        m_load(mat, first, slot).start()
        g_load(mat, first, slot).start()

    load(0, 0)
    barrier = pltpu.get_barrier_semaphore()
    for hop, flip in others:
        far_f, far_t = device(hop, flip)
        pl.semaphore_signal(barrier, inc=1, device_id={'fsdp': far_f, 'tp': far_t}, device_id_type=MESH)
    pl.semaphore_wait(barrier, 7)

    all_ref[me] = sq_ref[...]
    norm_copies = []
    for num, (hop, flip) in enumerate(others):
        far_f, far_t = device(hop, flip)
        copy = pltpu.make_async_remote_copy(
            src_ref=sq_ref, dst_ref=all_ref.at[me], send_sem=nsend.at[num], recv_sem=nrecv.at[num],
            device_id={'fsdp': far_f, 'tp': far_t}, device_id_type=MESH)
        copy.start()
        norm_copies.append(copy)
    for copy in norm_copies:
        copy.wait()
    total = all_ref[0]
    for dev in range(1, 8):
        total = total + all_ref[dev]
    norm = jnp.sqrt(total) + NORM_EPS
    mu = mu_ref[0]

    def x_copy(hop, flip, step, quarter):
        far_f, _ = device(hop, 0)
        far_x = (chip + chips[hop][1]) % 2
        far_t = 2 * far_x + (core + flip) % 2
        dst = out_ref.at[pl.ds(pl.multiple_of(fsdp * rows + quarter * CHUNK, CHUNK), CHUNK),
                         pl.ds(pl.multiple_of(tp * cols, cols), cols)]
        return pltpu.make_async_remote_copy(
            src_ref=x_buf.at[step], dst_ref=dst, send_sem=send_sem.at[hop, flip, quarter],
            recv_sem=recv_sem.at[hop, flip, quarter], device_id={'fsdp': far_f, 'tp': far_t}, device_id_type=MESH)

    def own_copy(step, quarter):
        dst = out_ref.at[pl.ds(pl.multiple_of(fsdp * rows + quarter * CHUNK, CHUNK), CHUNK),
                         pl.ds(pl.multiple_of(tp * cols, cols), cols)]
        return pltpu.make_async_copy(x_buf.at[step], dst, send_sem.at[3, 0, quarter])

    def make(step, _):
        near, flip, quarter, mat, first = where(step)
        slot = step % 2
        m_load(mat, first, slot).wait()
        g_load(mat, first, slot).wait()

        @pl.when(step + 1 < steps)
        def _():
            load(step + 1, 1 - slot)

        grad = g_buf[slot].astype(F32)
        nesterov = grad + mu * (mu * m_buf[slot] + grad)
        scale = jnp.where(mat == 0, norm[0:1, 0:1], norm[1:2, 0:1])
        x_buf[step] = (nesterov / scale).astype(BF16)

        @pl.when(near == 0)
        def _():
            x_copy(0, flip, step, quarter).start()
            x_copy(1, flip, step, quarter).start()

        @pl.when(near == 1)
        def _():
            x_copy(2, flip, step, quarter).start()

            @pl.when(flip == 1)
            def _():
                x_copy(3, flip, step, quarter).start()

            @pl.when(flip == 0)
            def _():
                own_copy(step, quarter).start()

        return 0

    lax.fori_loop(0, steps, make, 0)
    for quarter in range(per):
        own_copy(2 * per + quarter, quarter).wait()
        for hop, flip in others:
            step = (hop // 2) * 2 * per + flip * per + quarter
            x_copy(hop, flip, step, quarter).wait()


def spread(mu, sq_sum, momentum, gradient):
    mats, rows, cols = momentum.shape
    rows = rows // 2
    dma = pltpu.SemaphoreType.DMA
    per = rows // CHUNK
    sq_tile = jnp.zeros((8, 128), F32).at[:mats].set(sq_sum[:, None])
    return pl.pallas_call(
        functools.partial(spread_kernel, rows, cols),
        out_shape=jax.ShapeDtypeStruct((2 * rows, 4 * cols), BF16),
        in_specs=[
            pl.BlockSpec(memory_space=pltpu.SMEM),
            pl.BlockSpec(memory_space=pltpu.VMEM),
            pl.BlockSpec(memory_space=pl.ANY),
            pl.BlockSpec(memory_space=pl.ANY),
        ],
        out_specs=pl.BlockSpec(memory_space=pl.ANY),
        scratch_shapes=[
            pltpu.VMEM((8, 8, 128), F32),
            pltpu.VMEM((2, CHUNK, cols), F32),
            pltpu.VMEM((2, CHUNK, cols), BF16),
            pltpu.VMEM((4 * per, CHUNK, cols), BF16),
            dma((2, 2)), dma((7,)), dma((7,)),
            dma((4, 2, per)), dma((4, 2, per)),
        ],
        compiler_params=pltpu.CompilerParams(collective_id=0, has_side_effects=True, vmem_limit_bytes=VMEM_LIMIT),
        name='spread',
    )(mu.reshape(1), sq_tile, momentum, gradient)


NUM_BLK = 6
SPLIT = 5
STEPS = NUM_BLK * (NUM_BLK + 1) // 2 - SPLIT
HALF = STEPS // 2


def poly_kernel(x_hbm, b_ref, x_ref, a_ref, part_ref, own_ref, sq_ref, got_ref, stage_ref,
                xsem, psend, precv, asend, arecv, csend, crecv, fsend, frecv, bloc, bsend, brecv):
    total = NUM_BLK * (NUM_BLK + 1) // 2
    side, _, chip, core = here()
    peer = {'fsdp': side, 'tp': 2 * chip + 1 - core}
    twin = {'fsdp': 1 - side, 'tp': 2 * (1 - chip) + core}

    def x_load(pos):
        blk = pos + side * (4 * int(pos == 1) - int(pos > 1))
        return pltpu.make_async_copy(
            x_hbm.at[:, pl.ds(pl.multiple_of(blk * BLK, BLK), BLK)], x_ref.at[blk], xsem.at[pos])

    for pos in range(NUM_BLK):
        x_load(pos).start()
    barrier = pltpu.get_barrier_semaphore()
    for dev in (peer, twin):
        pl.semaphore_signal(barrier, inc=1, device_id=dev, device_id_type=MESH)
    pl.semaphore_wait(barrier, 2)

    def rows_of(blk):
        return pl.ds(pl.multiple_of(blk * BLK, BLK), BLK)

    def block(step, whose=None):
        whose = side if whose is None else whose
        early = (step < SPLIT) * jnp.int32(1)
        return tri_index(step + SPLIT * (early * whose + 1 - early), NUM_BLK)

    def copy_to(dev, src, dst, send, recv):
        return pltpu.make_async_remote_copy(
            src_ref=src, dst_ref=dst, send_sem=send, recv_sem=recv, device_id=dev, device_id_type=MESH)

    def part_copy(step):
        return copy_to(peer, part_ref, got_ref.at[step // 2], psend.at[step], precv.at[step])

    def region(row, col, flip):
        return a_ref.at[row, rows_of(col), :] if flip else a_ref.at[col, rows_of(row), :]

    def a_copy(step, flip):
        ref = region(*block(step), flip)
        return copy_to(peer, ref, ref, asend.at[flip, step], arecv.at[flip, step])

    def cross_copy(step, whose):
        ref = region(*block(step, whose), 0)
        return copy_to(twin, ref, ref, csend.at[step], crecv.at[step])

    def forward_copy(step, flip):
        ref = region(*block(step, 1 - side), flip)
        return copy_to(peer, ref, ref, fsend.at[flip, step], frecv.at[flip, step])

    def both(row, col, act):
        act(0)

        @pl.when(row != col)
        def _():
            act(1)

    def finish(step, slot):
        row, col = block(step)
        val = (own_ref[...] + got_ref[slot]).astype(BF16)
        a_ref[row, rows_of(col), :] = val.T
        a_ref[col, rows_of(row), :] = val

    def finish_send(step):
        @pl.when(step < SPLIT)
        def _():
            cross_copy(step, side).start()

        row, col = block(step)
        both(row, col, lambda flip: a_copy(step, flip).start())

    def receive(step):
        row, col = block(step, 1 - side)
        cross_copy(step, 1 - side).wait_recv()

        @pl.when(row != col)
        def _():
            a_ref[row, rows_of(col), :] = a_ref[col, rows_of(row), :].T

        both(row, col, lambda flip: forward_copy(step, flip).start())

    def product(step):
        row, col = block(step)
        return dot_tn(x_ref[row], x_ref[col])

    def gram(k, _):
        theirs = 2 * k + 1 - core
        own = 2 * k + core
        for late, first, last in ((0, 0, 3), (1, 3, 5), (2, 5, 6)):
            @pl.when(k == late)
            def _():
                for pos in range(first, last):
                    x_load(pos).wait()

        @pl.when(k >= 1)
        def _():
            part_copy(theirs - 2).wait_send()
            part_copy(own - 2).wait_recv()

        before = jnp.maximum(k - 1, 0)
        part_ref[...] = product(theirs)
        finish(2 * before + core, jnp.where(k == 0, HALF, before))
        part_copy(theirs).start()

        @pl.when(k >= 1)
        def _():
            finish_send(own - 2)

        for num in range(2):
            @pl.when(k == 5 + num)
            def _():
                receive(2 * num + core)

        own_ref[...] = product(own)
        return 0

    lax.fori_loop(0, HALF, gram, 0)
    part_copy(STEPS - 1 - core).wait_send()
    part_copy(STEPS - 2 + core).wait_recv()
    finish(STEPS - 2 + core, HALF - 1)
    finish_send(STEPS - 2 + core)

    @pl.when(core == 0)
    def _():
        receive(SPLIT - 1)

    def wait_got(k, _):
        step = 2 * k + 1 - core
        both(*block(step), lambda flip: a_copy(step, flip).wait_recv())
        return 0

    def wait_forward(k, _):
        step = 2 * k + 1 - core
        both(*block(step, 1 - side), lambda flip: forward_copy(step, flip).wait_recv())
        return 0

    lax.fori_loop(0, HALF, wait_got, 0)
    lax.fori_loop(0, 2 + core, wait_forward, 0)

    def b_copies(num, flip):
        row, col = tri_index(num, NUM_BLK)
        if flip:
            row, col = col, row
        src = stage_ref.at[(num // 2) % 2, flip]
        dst = b_ref.at[rows_of(row), rows_of(col)]
        local = pltpu.make_async_copy(src, dst, bloc.at[flip, num])
        return local, copy_to(peer, src, dst, bsend.at[flip, num], brecv.at[flip, num])

    def b_start(num):
        def act(flip):
            local, remote = b_copies(num, flip)
            remote.start()
            local.start()

        both(*tri_index(num, NUM_BLK), act)

    def b_drain(num):
        def act(flip):
            local, remote = b_copies(num, flip)
            local.wait()
            remote.wait_send()

        both(*tri_index(num, NUM_BLK), act)

    def combine(num, slot):
        row, col = tri_index(num, NUM_BLK)
        gram_sq = sq_ref[...].astype(BF16)
        val = a_ref[col, rows_of(row), :]
        val = (COEF_B * val.astype(F32) + COEF_C * gram_sq.astype(F32)).astype(BF16)
        stage_ref[slot, 0] = val
        stage_ref[slot, 1] = val.T

    num_mine = (total + 1) // 2 - core

    def square(k, _):
        num = 2 * k + core

        @pl.when(k >= 3)
        def _():
            b_drain(num - 6)

        combine(2 * jnp.maximum(k - 1, 0) + core, (k + 1) % 2)
        row, col = tri_index(num, NUM_BLK)
        sq_ref[...] = dot_tn(a_ref[row], a_ref[col])

        @pl.when(k >= 1)
        def _():
            b_start(num - 2)

        return 0

    lax.fori_loop(0, num_mine, square, 0)
    last = 2 * (num_mine - 1) + core
    b_drain(last - 4)
    combine(last, (num_mine - 1) % 2)
    b_start(last)

    def wait_sent(k, _):
        step = 2 * k + core
        both(*block(step), lambda flip: a_copy(step, flip).wait_send())
        return 0

    def wait_crossed(k, _):
        step = 2 * k + core
        cross_copy(step, side).wait_send()
        both(*block(step, 1 - side), lambda flip: forward_copy(step, flip).wait_send())
        return 0

    def wait_b(k, _):
        num = 2 * k + 1 - core
        both(*tri_index(num, NUM_BLK), lambda flip: b_copies(num, flip)[1].wait_recv())
        return 0

    lax.fori_loop(0, HALF, wait_sent, 0)
    lax.fori_loop(0, 3 - core, wait_crossed, 0)
    b_drain(last - 2)
    b_drain(last)
    lax.fori_loop(0, total - num_mine, wait_b, 0)


def poly(x_mat):
    rows, cols = x_mat.shape
    total = NUM_BLK * (NUM_BLK + 1) // 2
    dma = pltpu.SemaphoreType.DMA
    return pl.pallas_call(
        poly_kernel,
        out_shape=jax.ShapeDtypeStruct((cols, cols), BF16),
        in_specs=[pl.BlockSpec(memory_space=pl.ANY)],
        out_specs=pl.BlockSpec(memory_space=pl.ANY),
        scratch_shapes=[
            pltpu.VMEM((NUM_BLK, rows, BLK), BF16),
            pltpu.VMEM((NUM_BLK, cols, BLK), BF16),
            pltpu.VMEM((BLK, BLK), F32),
            pltpu.VMEM((BLK, BLK), F32),
            pltpu.VMEM((BLK, BLK), F32),
            pltpu.VMEM((HALF + 1, BLK, BLK), F32),
            pltpu.VMEM((2, 2, BLK, BLK), BF16),
            dma((NUM_BLK,)), dma((STEPS,)), dma((STEPS,)),
            dma((2, STEPS)), dma((2, STEPS)),
            dma((SPLIT,)), dma((SPLIT,)),
            dma((2, SPLIT)), dma((2, SPLIT)),
            dma((2, total)), dma((2, total)), dma((2, total)),
        ],
        compiler_params=pltpu.CompilerParams(
            collective_id=1, has_side_effects=True, vmem_limit_bytes=VMEM_LIMIT),
        name='poly',
    )(x_mat)


def update_kernel(tile, x_ref, b_ref, out_ref):
    blk = pl.program_id(0)
    upd = jnp.dot(x_ref[...], b_ref[...], preferred_element_type=F32)
    x_old = x_ref[:, pl.ds(pl.multiple_of(blk * tile, tile), tile)]
    out_ref[...] = (COEF_A * x_old.astype(F32) + upd).astype(BF16)


def update(x_mat, b_mat, row_tile=1024, col_tile=1024):
    rows, cols = x_mat.shape
    return pl.pallas_call(
        functools.partial(update_kernel, col_tile),
        grid=(cols // col_tile, rows // row_tile),
        out_shape=jax.ShapeDtypeStruct((rows, cols), BF16),
        in_specs=[
            pl.BlockSpec((row_tile, cols), lambda j, i: (i, 0)),
            pl.BlockSpec((cols, col_tile), lambda j, i: (0, j)),
        ],
        out_specs=pl.BlockSpec((row_tile, col_tile), lambda j, i: (i, j)),
        compiler_params=pltpu.CompilerParams(
            vmem_limit_bytes=VMEM_LIMIT, dimension_semantics=('arbitrary', 'arbitrary')),
        name='update',
    )(x_mat, b_mat)


def pair_kernel(tile, base, tab_ref, x_ref, b_ref, out0_ref, out1_ref):
    which = pl.program_id(0)
    blk = tab_ref[1, base + which]
    upd = jnp.dot(x_ref[...], b_ref[...], preferred_element_type=F32)
    x_old = x_ref[:, pl.ds(pl.multiple_of(blk * tile, tile), tile)]
    val = (COEF_A * x_old.astype(F32) + upd).astype(BF16)

    @pl.when(which == 0)
    def _():
        out0_ref[...] = val

    @pl.when(which == 1)
    def _():
        out1_ref[...] = val


def last_pieces(x_mat, b_mat, table, base, piece_rows, row_tile=1024):
    _, cols = x_mat.shape
    tile = cols // 4
    last = piece_rows // row_tile - 1
    return pl.pallas_call(
        functools.partial(pair_kernel, tile, base),
        grid_spec=pltpu.PrefetchScalarGridSpec(
            num_scalar_prefetch=1,
            grid=(2, last + 1),
            in_specs=[
                pl.BlockSpec((row_tile, cols), lambda p, i, tab: (tab[0, base + p] + i, 0)),
                pl.BlockSpec((cols, tile), lambda p, i, tab: (0, tab[1, base + p])),
            ],
            out_specs=[
                pl.BlockSpec((row_tile, tile), lambda p, i, tab: (i * (1 - p) + last * p, 0)),
                pl.BlockSpec((row_tile, tile), lambda p, i, tab: (i * p, 0)),
            ],
        ),
        out_shape=[jax.ShapeDtypeStruct((piece_rows, tile), BF16)] * 2,
        compiler_params=pltpu.CompilerParams(
            vmem_limit_bytes=VMEM_LIMIT, dimension_semantics=('arbitrary', 'arbitrary')),
        cost_estimate=pl.CostEstimate(
            flops=4 * piece_rows * tile * cols, bytes_accessed=4 * cols * (piece_rows + tile), transcendentals=0),
        name='last_pieces',
    )(table, x_mat, b_mat)


def apply_kernel(tab_ref, scale_ref, w_ref, x_ref, *rest):
    rest[-1][0] = scale_ref[0] * w_ref[0] - scale_ref[1] * x_ref[...].astype(F32)


def apply_piece(weight, x_piece, scales, table, base, so_far, row_tile=512):
    rows, cols = x_piece.shape
    extra = [] if so_far is None else [so_far]
    w_spec = pl.BlockSpec((1, row_tile, cols), lambda i, tab: (tab[0, base], tab[1, base] + i, 0))
    return pl.pallas_call(
        apply_kernel,
        grid_spec=pltpu.PrefetchScalarGridSpec(
            num_scalar_prefetch=1,
            grid=(rows // row_tile,),
            in_specs=[
                pl.BlockSpec(memory_space=pltpu.SMEM),
                w_spec,
                pl.BlockSpec((row_tile, cols), lambda i, tab: (i, 0)),
            ] + [pl.BlockSpec(memory_space=pl.ANY)] * len(extra),
            out_specs=w_spec,
        ),
        out_shape=jax.ShapeDtypeStruct(weight.shape, F32),
        input_output_aliases={4: 0} if extra else {},
        compiler_params=pltpu.CompilerParams(vmem_limit_bytes=VMEM_LIMIT, dimension_semantics=('arbitrary',)),
        cost_estimate=pl.CostEstimate(flops=3 * rows * cols, bytes_accessed=10 * rows * cols, transcendentals=0),
        name='apply_piece',
    )(table, scales, weight, x_piece, *extra)


def solution(mesh):
    fsdp_size = mesh.shape['fsdp']
    mat_spec = P('stage', 'fsdp', 'tp')
    scalar_spec = P()

    def local_step(weight, momentum, gradient, learn_rate, mom_coef, weight_decay):
        row_dim = weight.shape[1] * fsdp_size
        fsdp, _, chip, core = here()
        grad_full = gradient.astype(F32)
        mom_new = mom_coef * momentum + grad_full
        nesterov = grad_full + mom_coef * mom_new
        sq_sum = jnp.sum(nesterov * nesterov, axis=(1, 2))
        sub = row_dim // 4
        half = sub // 2
        mat = (fsdp + chip) % 2
        far = 1 - mat
        r_here, r_far = fsdp * (sub // 1024), (1 - fsdp) * (sub // 1024)
        step = half // 1024
        x_col, y_col = 2 * (1 - chip) + core, 2 * chip + 1 - core
        piece_tab = jnp.stack([
            jnp.stack([r_here, r_far, r_here + step, r_far + step, r_here, r_here]),
            jnp.stack([x_col, y_col, x_col, y_col, y_col, 2 * chip + core]),
        ]).astype(jnp.int32)
        c_here, c_far = core * (sub // 512), (1 - core) * (sub // 512)
        step = half // 512
        apply_tab = jnp.stack([
            jnp.stack([mat, mat, far, far, far, far]),
            jnp.stack([c_here, c_far, c_here, c_far, c_here + step, c_far + step]),
        ]).astype(jnp.int32)
        scales = jnp.stack([1.0 - learn_rate * weight_decay, learn_rate * 0.2 * math.sqrt(row_dim)])
        sq_sum, piece_tab, apply_tab, scales = lax.optimization_barrier((sq_sum, piece_tab, apply_tab, scales))
        x_mat = spread(mom_coef, sq_sum, momentum, gradient)
        for _ in range(NS_STEPS - 1):
            x_mat = update(x_mat, poly(x_mat))
        b_mat = poly(x_mat)

        def permute(piece, kind):
            pairs = []
            for src in range(8):
                f_src, t_src = src // 4, src % 4
                if kind == 'x':
                    dst = f_src * 4 + (t_src + 2) % 4
                elif kind == 'y':
                    dst = (1 - f_src) * 4 + t_src + 1 - 2 * (t_src % 2)
                else:
                    dst = f_src * 4 + t_src + 1 - 2 * (t_src % 2)
                pairs.append((src, dst))
            return lax.ppermute(piece, ('fsdp', 'tp'), pairs)

        moved = []
        tie = b_mat
        for part in range(2):
            to_x, to_y = last_pieces(x_mat, tie, piece_tab, 2 * part, half)
            moved.append(permute(to_x, 'x'))
            moved.append(permute(to_y, 'y'))
            tie, _, _ = lax.optimization_barrier((tie, to_x, to_y))
        near, own = last_pieces(x_mat, tie, piece_tab, 4, sub)
        near = permute(near, 'core')
        new_weight = apply_piece(weight, own, scales, apply_tab, 0, None)
        new_weight = apply_piece(weight, near, scales, apply_tab, 1, new_weight)
        for num, x_piece in enumerate(moved):
            new_weight = apply_piece(weight, x_piece, scales, apply_tab, 2 + num, new_weight)
        return new_weight, mom_new

    return jax.shard_map(local_step, mesh=mesh, in_specs=(mat_spec,) * 3 + (scalar_spec,) * 3, out_specs=(mat_spec, mat_spec), check_vma=False)
```

```python
import functools
import math

import jax
import jax.numpy as jnp
from jax import lax
from jax.experimental import pallas as pl
from jax.experimental.pallas import tpu as pltpu
from jax.sharding import PartitionSpec as P


NS_STEPS = 5
COEF_A = 3.4445
COEF_B = -4.7750
COEF_C = 2.0315
NORM_EPS = 1e-7


MESH = pl.DeviceIdType.MESH
F32 = jnp.float32
BF16 = jnp.bfloat16

BLK = 512
VMEM_LIMIT = 64 * 1024 * 1024 - 65536


def here():
    fsdp = lax.axis_index('fsdp')
    tp = lax.axis_index('tp')
    return fsdp, tp, tp // 2, tp % 2


def tri_index(step, num_blk):
    step = jnp.asarray(step, jnp.int32)
    row = jnp.int32(0)
    start = jnp.int32(0)
    first = 0
    for blk in range(1, num_blk):
        first += num_blk - blk + 1
        past = (step >= first).astype(jnp.int32)
        row = row + past
        start = start + past * (num_blk - blk + 1)
    return row, step - start + row


def dot_tn(lhs, rhs):
    return lax.dot_general(lhs, rhs, (((0,), (0,)), ((), ())), preferred_element_type=F32)


CHUNK = 512


def spread_kernel(rows, cols, mu_ref, sq_ref, m_ref, g_ref, out_ref, all_ref, m_buf, g_buf, x_buf,
                  load_sem, nsend, nrecv, send_sem, recv_sem):
    fsdp, tp, chip, core = here()
    me = 4 * fsdp + tp
    per = rows // CHUNK
    steps = 4 * per
    chips = ((0, 1), (1, 0), (1, 1), (0, 0))

    def device(hop, flip):
        far_f = (fsdp + chips[hop][0]) % 2
        far_x = (chip + chips[hop][1]) % 2
        far_c = (core + flip) % 2
        return far_f, 2 * far_x + far_c

    others = [(hop, flip) for hop in range(4) for flip in range(2) if (hop, flip) != (3, 0)]

    def m_load(mat, first, slot):
        return pltpu.make_async_copy(m_ref.at[mat, pl.ds(first, CHUNK), :], m_buf.at[slot], load_sem.at[0, slot])

    def g_load(mat, first, slot):
        return pltpu.make_async_copy(g_ref.at[mat, pl.ds(first, CHUNK), :], g_buf.at[slot], load_sem.at[1, slot])

    def where(step):
        near = step // (2 * per)
        flip = (step // per) % 2
        quarter = step % per
        mat = (fsdp + chip + 1 - near) % 2
        far_c = (core + flip) % 2
        first = pl.multiple_of(far_c * rows + quarter * CHUNK, CHUNK)
        return near, flip, quarter, mat, first

    def load(step, slot):
        _, _, _, mat, first = where(step)
        m_load(mat, first, slot).start()
        g_load(mat, first, slot).start()

    load(0, 0)
    barrier = pltpu.get_barrier_semaphore()
    for hop, flip in others:
        far_f, far_t = device(hop, flip)
        pl.semaphore_signal(barrier, inc=1, device_id={'fsdp': far_f, 'tp': far_t}, device_id_type=MESH)
    pl.semaphore_wait(barrier, 7)

    all_ref[me] = sq_ref[...]
    norm_copies = []
    for num, (hop, flip) in enumerate(others):
        far_f, far_t = device(hop, flip)
        copy = pltpu.make_async_remote_copy(
            src_ref=sq_ref, dst_ref=all_ref.at[me], send_sem=nsend.at[num], recv_sem=nrecv.at[num],
            device_id={'fsdp': far_f, 'tp': far_t}, device_id_type=MESH)
        copy.start()
        norm_copies.append(copy)
    for copy in norm_copies:
        copy.wait()
    total = all_ref[0]
    for dev in range(1, 8):
        total = total + all_ref[dev]
    norm = jnp.sqrt(total) + NORM_EPS
    mu = mu_ref[0]

    def x_copy(hop, flip, step, quarter):
        far_f, _ = device(hop, 0)
        far_x = (chip + chips[hop][1]) % 2
        far_t = 2 * far_x + (core + flip) % 2
        dst = out_ref.at[pl.ds(pl.multiple_of(fsdp * rows + quarter * CHUNK, CHUNK), CHUNK),
                         pl.ds(pl.multiple_of(tp * cols, cols), cols)]
        return pltpu.make_async_remote_copy(
            src_ref=x_buf.at[step], dst_ref=dst, send_sem=send_sem.at[hop, flip, quarter],
            recv_sem=recv_sem.at[hop, flip, quarter], device_id={'fsdp': far_f, 'tp': far_t}, device_id_type=MESH)

    def own_copy(step, quarter):
        dst = out_ref.at[pl.ds(pl.multiple_of(fsdp * rows + quarter * CHUNK, CHUNK), CHUNK),
                         pl.ds(pl.multiple_of(tp * cols, cols), cols)]
        return pltpu.make_async_copy(x_buf.at[step], dst, send_sem.at[3, 0, quarter])

    def make(step, _):
        near, flip, quarter, mat, first = where(step)
        slot = step % 2
        m_load(mat, first, slot).wait()
        g_load(mat, first, slot).wait()

        @pl.when(step + 1 < steps)
        def _():
            load(step + 1, 1 - slot)

        grad = g_buf[slot].astype(F32)
        nesterov = grad + mu * (mu * m_buf[slot] + grad)
        scale = jnp.where(mat == 0, norm[0:1, 0:1], norm[1:2, 0:1])
        x_buf[step] = (nesterov / scale).astype(BF16)

        @pl.when(near == 0)
        def _():
            x_copy(0, flip, step, quarter).start()
            x_copy(1, flip, step, quarter).start()

        @pl.when(near == 1)
        def _():
            x_copy(2, flip, step, quarter).start()

            @pl.when(flip == 1)
            def _():
                x_copy(3, flip, step, quarter).start()

            @pl.when(flip == 0)
            def _():
                own_copy(step, quarter).start()

        return 0

    lax.fori_loop(0, steps, make, 0)
    for quarter in range(per):
        own_copy(2 * per + quarter, quarter).wait()
        for hop, flip in others:
            step = (hop // 2) * 2 * per + flip * per + quarter
            x_copy(hop, flip, step, quarter).wait()


def spread(mu, sq_sum, momentum, gradient):
    mats, rows, cols = momentum.shape
    rows = rows // 2
    dma = pltpu.SemaphoreType.DMA
    per = rows // CHUNK
    sq_tile = jnp.zeros((8, 128), F32).at[:mats].set(sq_sum[:, None])
    return pl.pallas_call(
        functools.partial(spread_kernel, rows, cols),
        out_shape=jax.ShapeDtypeStruct((2 * rows, 4 * cols), BF16),
        in_specs=[
            pl.BlockSpec(memory_space=pltpu.SMEM),
            pl.BlockSpec(memory_space=pltpu.VMEM),
            pl.BlockSpec(memory_space=pl.ANY),
            pl.BlockSpec(memory_space=pl.ANY),
        ],
        out_specs=pl.BlockSpec(memory_space=pl.ANY),
        scratch_shapes=[
            pltpu.VMEM((8, 8, 128), F32),
            pltpu.VMEM((2, CHUNK, cols), F32),
            pltpu.VMEM((2, CHUNK, cols), BF16),
            pltpu.VMEM((4 * per, CHUNK, cols), BF16),
            dma((2, 2)), dma((7,)), dma((7,)),
            dma((4, 2, per)), dma((4, 2, per)),
        ],
        compiler_params=pltpu.CompilerParams(collective_id=0, has_side_effects=True, vmem_limit_bytes=VMEM_LIMIT),
        name='spread',
    )(mu.reshape(1), sq_tile, momentum, gradient)


NUM_BLK = 6
SPLIT = 5
STEPS = NUM_BLK * (NUM_BLK + 1) // 2 - SPLIT
HALF = STEPS // 2


def poly_kernel(x_hbm, b_ref, x_ref, a_ref, part_ref, own_ref, sq_ref, got_ref, stage_ref,
                xsem, psend, precv, asend, arecv, csend, crecv, fsend, frecv, bloc, bsend, brecv):
    total = NUM_BLK * (NUM_BLK + 1) // 2
    side, _, chip, core = here()
    peer = {'fsdp': side, 'tp': 2 * chip + 1 - core}
    twin = {'fsdp': 1 - side, 'tp': 2 * (1 - chip) + core}

    def x_load(pos):
        other = (1 - core, 5 * core, 5 - 4 * core, 2, 3, 4)[pos]
        blk = pos * (1 - side) + other * side
        return pltpu.make_async_copy(
            x_hbm.at[:, pl.ds(pl.multiple_of(blk * BLK, BLK), BLK)], x_ref.at[blk], xsem.at[pos])

    for pos in range(NUM_BLK):
        x_load(pos).start()
    barrier = pltpu.get_barrier_semaphore()
    for dev in (peer, twin):
        pl.semaphore_signal(barrier, inc=1, device_id=dev, device_id_type=MESH)
    pl.semaphore_wait(barrier, 2)

    def rows_of(blk):
        return pl.ds(pl.multiple_of(blk * BLK, BLK), BLK)

    def block(step, whose=None):
        whose = side if whose is None else whose
        early = (step < SPLIT) * jnp.int32(1)
        return tri_index(step + SPLIT * (early * whose + 1 - early), NUM_BLK)

    def copy_to(dev, src, dst, send, recv):
        return pltpu.make_async_remote_copy(
            src_ref=src, dst_ref=dst, send_sem=send, recv_sem=recv, device_id=dev, device_id_type=MESH)

    def part_copy(step):
        return copy_to(peer, part_ref, got_ref.at[step // 2], psend.at[step], precv.at[step])

    def region(row, col, flip):
        return a_ref.at[row, rows_of(col), :] if flip else a_ref.at[col, rows_of(row), :]

    def a_copy(step, flip):
        ref = region(*block(step), flip)
        return copy_to(peer, ref, ref, asend.at[flip, step], arecv.at[flip, step])

    def cross_copy(step, whose):
        ref = region(*block(step, whose), 0)
        return copy_to(twin, ref, ref, csend.at[step], crecv.at[step])

    def forward_copy(step, flip):
        ref = region(*block(step, 1 - side), flip)
        return copy_to(peer, ref, ref, fsend.at[flip, step], frecv.at[flip, step])

    def both(row, col, act):
        act(0)

        @pl.when(row != col)
        def _():
            act(1)

    def finish(step, slot):
        row, col = block(step)
        val = (own_ref[...] + got_ref[slot]).astype(BF16)
        a_ref[row, rows_of(col), :] = val.T
        a_ref[col, rows_of(row), :] = val

    def finish_send(step):
        @pl.when(step < SPLIT)
        def _():
            cross_copy(step, side).start()

        row, col = block(step)
        both(row, col, lambda flip: a_copy(step, flip).start())

    def receive(step):
        row, col = block(step, 1 - side)
        cross_copy(step, 1 - side).wait_recv()

        @pl.when(row != col)
        def _():
            a_ref[row, rows_of(col), :] = a_ref[col, rows_of(row), :].T

        both(row, col, lambda flip: forward_copy(step, flip).start())

    def product(step):
        row, col = block(step)
        return dot_tn(x_ref[row], x_ref[col])

    def gram(k, _):
        theirs = 2 * k + 1 - core
        own = 2 * k + core
        for late, first, last in ((0, 0, 2), (1, 3, 5), (2, 5, 6)):
            @pl.when(k == late)
            def _():
                for pos in range(first, last):
                    x_load(pos).wait()

        @pl.when(k >= 1)
        def _():
            part_copy(theirs - 2).wait_send()
            part_copy(own - 2).wait_recv()

        before = jnp.maximum(k - 1, 0)
        part_ref[...] = product(theirs)
        finish(2 * before + core, jnp.where(k == 0, HALF, before))
        part_copy(theirs).start()

        @pl.when(k >= 1)
        def _():
            finish_send(own - 2)

        for num in range(2):
            @pl.when(k == 5 + num)
            def _():
                receive(2 * num + core)

        @pl.when(k == 0)
        def _():
            x_load(2).wait()

        own_ref[...] = product(own)
        return 0

    lax.fori_loop(0, HALF, gram, 0)
    part_copy(STEPS - 1 - core).wait_send()
    part_copy(STEPS - 2 + core).wait_recv()
    finish(STEPS - 2 + core, HALF - 1)
    finish_send(STEPS - 2 + core)

    @pl.when(core == 0)
    def _():
        receive(SPLIT - 1)

    def wait_got(k, _):
        step = 2 * k + 1 - core
        both(*block(step), lambda flip: a_copy(step, flip).wait_recv())
        return 0

    def wait_forward(k, _):
        step = 2 * k + 1 - core
        both(*block(step, 1 - side), lambda flip: forward_copy(step, flip).wait_recv())
        return 0

    lax.fori_loop(0, HALF, wait_got, 0)
    lax.fori_loop(0, 2 + core, wait_forward, 0)

    def b_copies(num, flip):
        row, col = tri_index(num, NUM_BLK)
        if flip:
            row, col = col, row
        src = stage_ref.at[(num // 2) % 2, flip]
        dst = b_ref.at[rows_of(row), rows_of(col)]
        local = pltpu.make_async_copy(src, dst, bloc.at[flip, num])
        return local, copy_to(peer, src, dst, bsend.at[flip, num], brecv.at[flip, num])

    def b_start(num):
        def act(flip):
            local, remote = b_copies(num, flip)
            remote.start()
            local.start()

        both(*tri_index(num, NUM_BLK), act)

    def b_drain(num):
        def act(flip):
            local, remote = b_copies(num, flip)
            local.wait()
            remote.wait_send()

        both(*tri_index(num, NUM_BLK), act)

    def combine(num, slot):
        row, col = tri_index(num, NUM_BLK)
        gram_sq = sq_ref[...].astype(BF16)
        val = a_ref[col, rows_of(row), :]
        val = (COEF_B * val.astype(F32) + COEF_C * gram_sq.astype(F32)).astype(BF16)
        stage_ref[slot, 0] = val
        stage_ref[slot, 1] = val.T

    num_mine = (total + 1) // 2 - core

    def square(k, _):
        num = 2 * k + core

        @pl.when(k >= 3)
        def _():
            b_drain(num - 6)

        combine(2 * jnp.maximum(k - 1, 0) + core, (k + 1) % 2)
        row, col = tri_index(num, NUM_BLK)
        sq_ref[...] = dot_tn(a_ref[row], a_ref[col])

        @pl.when(k >= 1)
        def _():
            b_start(num - 2)

        return 0

    lax.fori_loop(0, num_mine, square, 0)
    last = 2 * (num_mine - 1) + core
    b_drain(last - 4)
    combine(last, (num_mine - 1) % 2)
    b_start(last)

    def wait_sent(k, _):
        step = 2 * k + core
        both(*block(step), lambda flip: a_copy(step, flip).wait_send())
        return 0

    def wait_crossed(k, _):
        step = 2 * k + core
        cross_copy(step, side).wait_send()
        both(*block(step, 1 - side), lambda flip: forward_copy(step, flip).wait_send())
        return 0

    def wait_b(k, _):
        num = 2 * k + 1 - core
        both(*tri_index(num, NUM_BLK), lambda flip: b_copies(num, flip)[1].wait_recv())
        return 0

    lax.fori_loop(0, HALF, wait_sent, 0)
    lax.fori_loop(0, 3 - core, wait_crossed, 0)
    b_drain(last - 2)
    b_drain(last)
    lax.fori_loop(0, total - num_mine, wait_b, 0)


def poly(x_mat):
    rows, cols = x_mat.shape
    total = NUM_BLK * (NUM_BLK + 1) // 2
    dma = pltpu.SemaphoreType.DMA
    return pl.pallas_call(
        poly_kernel,
        out_shape=jax.ShapeDtypeStruct((cols, cols), BF16),
        in_specs=[pl.BlockSpec(memory_space=pl.ANY)],
        out_specs=pl.BlockSpec(memory_space=pl.ANY),
        scratch_shapes=[
            pltpu.VMEM((NUM_BLK, rows, BLK), BF16),
            pltpu.VMEM((NUM_BLK, cols, BLK), BF16),
            pltpu.VMEM((BLK, BLK), F32),
            pltpu.VMEM((BLK, BLK), F32),
            pltpu.VMEM((BLK, BLK), F32),
            pltpu.VMEM((HALF + 1, BLK, BLK), F32),
            pltpu.VMEM((2, 2, BLK, BLK), BF16),
            dma((NUM_BLK,)), dma((STEPS,)), dma((STEPS,)),
            dma((2, STEPS)), dma((2, STEPS)),
            dma((SPLIT,)), dma((SPLIT,)),
            dma((2, SPLIT)), dma((2, SPLIT)),
            dma((2, total)), dma((2, total)), dma((2, total)),
        ],
        compiler_params=pltpu.CompilerParams(
            collective_id=1, has_side_effects=True, vmem_limit_bytes=VMEM_LIMIT),
        name='poly',
    )(x_mat)


def update_kernel(tile, x_ref, b_ref, out_ref):
    blk = pl.program_id(0)
    upd = jnp.dot(x_ref[...], b_ref[...], preferred_element_type=F32)
    x_old = x_ref[:, pl.ds(pl.multiple_of(blk * tile, tile), tile)]
    out_ref[...] = (COEF_A * x_old.astype(F32) + upd).astype(BF16)


def update(x_mat, b_mat, row_tile=1024, col_tile=1024):
    rows, cols = x_mat.shape
    return pl.pallas_call(
        functools.partial(update_kernel, col_tile),
        grid=(cols // col_tile, rows // row_tile),
        out_shape=jax.ShapeDtypeStruct((rows, cols), BF16),
        in_specs=[
            pl.BlockSpec((row_tile, cols), lambda j, i: (i, 0)),
            pl.BlockSpec((cols, col_tile), lambda j, i: (0, j)),
        ],
        out_specs=pl.BlockSpec((row_tile, col_tile), lambda j, i: (i, j)),
        compiler_params=pltpu.CompilerParams(
            vmem_limit_bytes=VMEM_LIMIT, dimension_semantics=('arbitrary', 'arbitrary')),
        name='update',
    )(x_mat, b_mat)


def pair_kernel(tile, base, tab_ref, x_ref, b_ref, out0_ref, out1_ref):
    which = pl.program_id(0)
    blk = tab_ref[1, base + which]
    upd = jnp.dot(x_ref[...], b_ref[...], preferred_element_type=F32)
    x_old = x_ref[:, pl.ds(pl.multiple_of(blk * tile, tile), tile)]
    val = (COEF_A * x_old.astype(F32) + upd).astype(BF16)

    @pl.when(which == 0)
    def _():
        out0_ref[...] = val

    @pl.when(which == 1)
    def _():
        out1_ref[...] = val


def last_pieces(x_mat, b_mat, table, base, piece_rows, row_tile=512):
    _, cols = x_mat.shape
    tile = cols // 4
    last = piece_rows // row_tile - 1
    return pl.pallas_call(
        functools.partial(pair_kernel, tile, base),
        grid_spec=pltpu.PrefetchScalarGridSpec(
            num_scalar_prefetch=1,
            grid=(2, last + 1),
            in_specs=[
                pl.BlockSpec((row_tile, cols), lambda p, i, tab: (tab[0, base + p] + i, 0)),
                pl.BlockSpec((cols, tile), lambda p, i, tab: (0, tab[1, base + p])),
            ],
            out_specs=[
                pl.BlockSpec((row_tile, tile), lambda p, i, tab: (i * (1 - p) + last * p, 0)),
                pl.BlockSpec((row_tile, tile), lambda p, i, tab: (i * p, 0)),
            ],
        ),
        out_shape=[jax.ShapeDtypeStruct((piece_rows, tile), BF16)] * 2,
        compiler_params=pltpu.CompilerParams(
            vmem_limit_bytes=VMEM_LIMIT, dimension_semantics=('arbitrary', 'arbitrary')),
        cost_estimate=pl.CostEstimate(
            flops=4 * piece_rows * tile * cols, bytes_accessed=4 * cols * (piece_rows + tile), transcendentals=0),
        name='last_pieces',
    )(table, x_mat, b_mat)


def apply_kernel(tab_ref, scale_ref, w_ref, x_ref, *rest):
    rest[-1][0] = scale_ref[0] * w_ref[0] - scale_ref[1] * x_ref[...].astype(F32)


def apply_piece(weight, x_piece, scales, table, base, so_far, row_tile=512):
    rows, cols = x_piece.shape
    extra = [] if so_far is None else [so_far]
    w_spec = pl.BlockSpec((1, row_tile, cols), lambda i, tab: (tab[0, base], tab[1, base] + i, 0))
    return pl.pallas_call(
        apply_kernel,
        grid_spec=pltpu.PrefetchScalarGridSpec(
            num_scalar_prefetch=1,
            grid=(rows // row_tile,),
            in_specs=[
                pl.BlockSpec(memory_space=pltpu.SMEM),
                w_spec,
                pl.BlockSpec((row_tile, cols), lambda i, tab: (i, 0)),
            ] + [pl.BlockSpec(memory_space=pl.ANY)] * len(extra),
            out_specs=w_spec,
        ),
        out_shape=jax.ShapeDtypeStruct(weight.shape, F32),
        input_output_aliases={4: 0} if extra else {},
        compiler_params=pltpu.CompilerParams(vmem_limit_bytes=VMEM_LIMIT, dimension_semantics=('arbitrary',)),
        cost_estimate=pl.CostEstimate(flops=3 * rows * cols, bytes_accessed=10 * rows * cols, transcendentals=0),
        name='apply_piece',
    )(table, scales, weight, x_piece, *extra)


def solution(mesh):
    fsdp_size = mesh.shape['fsdp']
    mat_spec = P('stage', 'fsdp', 'tp')
    scalar_spec = P()

    def local_step(weight, momentum, gradient, learn_rate, mom_coef, weight_decay):
        row_dim = weight.shape[1] * fsdp_size
        fsdp, _, chip, core = here()
        grad_full = gradient.astype(F32)
        mom_new = mom_coef * momentum + grad_full
        nesterov = grad_full + mom_coef * mom_new
        sq_sum = jnp.sum(nesterov * nesterov, axis=(1, 2))
        sub = row_dim // 4
        half = sub // 2
        mat = (fsdp + chip) % 2
        far = 1 - mat
        r_here, r_far = fsdp * (sub // 512), (1 - fsdp) * (sub // 512)
        step = half // 512
        x_col, y_col = 2 * (1 - chip) + core, 2 * chip + 1 - core
        piece_tab = jnp.stack([
            jnp.stack([r_here, r_far, r_here + step, r_far + step, r_here, r_here]),
            jnp.stack([x_col, y_col, x_col, y_col, y_col, 2 * chip + core]),
        ]).astype(jnp.int32)
        c_here, c_far = core * (sub // 512), (1 - core) * (sub // 512)
        step = half // 512
        apply_tab = jnp.stack([
            jnp.stack([mat, mat, far, far, far, far]),
            jnp.stack([c_here, c_far, c_here, c_far, c_here + step, c_far + step]),
        ]).astype(jnp.int32)
        scales = jnp.stack([1.0 - learn_rate * weight_decay, learn_rate * 0.2 * math.sqrt(row_dim)])
        sq_sum, piece_tab, apply_tab, scales = lax.optimization_barrier((sq_sum, piece_tab, apply_tab, scales))
        x_mat = spread(mom_coef, sq_sum, momentum, gradient)
        for _ in range(NS_STEPS - 1):
            x_mat = update(x_mat, poly(x_mat))
        b_mat = poly(x_mat)

        def permute(piece, kind):
            pairs = []
            for src in range(8):
                f_src, t_src = src // 4, src % 4
                if kind == 'x':
                    dst = f_src * 4 + (t_src + 2) % 4
                elif kind == 'y':
                    dst = (1 - f_src) * 4 + t_src + 1 - 2 * (t_src % 2)
                else:
                    dst = f_src * 4 + t_src + 1 - 2 * (t_src % 2)
                pairs.append((src, dst))
            return lax.ppermute(piece, ('fsdp', 'tp'), pairs)

        moved = []
        tie = b_mat
        for part in range(2):
            to_x, to_y = last_pieces(x_mat, tie, piece_tab, 2 * part, half)
            moved.append(permute(to_x, 'x'))
            moved.append(permute(to_y, 'y'))
            tie, _, _ = lax.optimization_barrier((tie, to_x, to_y))
        near, own = last_pieces(x_mat, tie, piece_tab, 4, sub)
        near = permute(near, 'core')
        new_weight = apply_piece(weight, own, scales, apply_tab, 0, None)
        new_weight = apply_piece(weight, near, scales, apply_tab, 1, new_weight)
        for num, x_piece in enumerate(moved):
            new_weight = apply_piece(weight, x_piece, scales, apply_tab, 2 + num, new_weight)
        return new_weight, mom_new

    return jax.shard_map(local_step, mesh=mesh, in_specs=(mat_spec,) * 3 + (scalar_spec,) * 3, out_specs=(mat_spec, mat_spec), check_vma=False)
```
